512 devices in a mesh: row: 16 (over z), col: 32 (over x, y, core).
Axes of the slice: x: 4, y: 4, z: 16, core: 2. Of those that a mesh axis runs over, the one named last changes fastest.
Arguments:
- slab_left: bfloat16 [64, 32, 2048, 32], P('row', 'col'), may hold values from -6 to 6
- slab_right: bfloat16 [64, 32, 2048, 32], P('row', 'col'), may hold values from -1 to 1
- slab_ranks: int32 [64, 32], P('row', 'col'), may hold values from 20 to 32
- panel_left: bfloat16 [64, 2048, 32], P('row', 'col'), may hold values from -6 to 6
- panel_right: bfloat16 [64, 2048, 32], P('row', 'col'), may hold values from -0.125 to 0.125
- panel_ranks: int32 [64], P('row'), may hold values from 20 to 32
- inverse_factor: bfloat16 [2048, 2048], P(None, 'col'), may hold values from -2 to 2, as said below
- sketch: bfloat16 [2048, 32], replicated, may hold values from -6 to 6
Outputs:
- new_left: bfloat16 [64, 32, 2048, 32], P('row', 'col')
- new_right: bfloat16 [64, 32, 2048, 32], P('row', 'col')
The draws below stay inside these ranges and needn't reach their ends.
Inputs may be any that keep to these rules, and one draw needn't show every extreme that they name: `slab_ranks`: number of live columns of a slab tile's factors; columns from that index on are padding. `panel_ranks`: number of live columns of a panel tile's factors; columns from that index on are padding. `inverse_factor`: lower triangular: entries above the diagonal are zero, diagonal entries positive.
All inputs are finite; a program needn't handle non-finite values.
Results may differ from the reference program's by a relative error of at most 0.0073.
Values may be sent and summed in bfloat16 or wider, within the bound.
A program may use at most 64 MiB of HBM per device.

```python
import math
import jax
import jax.numpy as jnp
from jax import lax

B = 2048
R = 32
TR = 4
MT = 64
NT = 32
N_ROW = 16
N_COL = 32


def draw_inverse_factor(key, part):
    first_key = jax.random.fold_in(key, 11)
    second_key = jax.random.fold_in(key, 12)
    diagonal = jax.random.uniform(first_key, (B,), jnp.float32, 0.5, 1.5)
    spread = 1.0
    below_part = jnp.clip(jax.random.normal(second_key, (B, B), jnp.float32), -6.0, 6.0) * (spread / math.sqrt(B))
    lower_part = jnp.tril(below_part, -1) + jnp.diag(diagonal)
    return lower_part.astype(jnp.bfloat16)


def set_ends(result, key, low, high):
    longest = result.shape.index(max(result.shape))
    spots = []
    for shift in (0, 1):
        where = [jax.random.randint(jax.random.fold_in(key, axis), (), 0, length) for axis, length in enumerate(result.shape)]
        where[longest] = (where[longest] + shift) % result.shape[longest]
        spots.append(tuple(where))
    return result.at[spots[0]].set(low).at[spots[1]].set(high)


def levels(own_key, dims, split, least, top_value):
    factor_of, own = 1.0, jax.random.fold_in(own_key, 6)
    for position, parts in split:
        steps = jnp.exp(jax.random.uniform(jax.random.fold_in(own, position), (parts,), jnp.float32, least / len(split), top_value / len(split)))
        factor_of = factor_of * jnp.repeat(steps, dims[position] // parts).reshape([-1 if axis == position else 1 for axis in range(len(dims))])
    return factor_of


def gaussian(rng, extent, scale, bound, pieces=(), kind=jnp.bfloat16):
    result = jax.random.normal(rng, extent, jnp.float32) * scale
    if len(pieces) > 0:
        result = levels(rng, extent, pieces, -0.22, 0.18) * result
    return jnp.clip(result, min=-bound, max=bound).astype(kind)


def setup_inputs(seed: int = 0) -> dict:
    splits = jax.random.split(jax.random.key(seed), 9)
    return {
        "slab_left": gaussian(splits[0], (MT, NT, B, R), 1.0, 6.0, ((0, 16), (1, 32))),
        "slab_right": gaussian(splits[1], (MT, NT, B, R), R ** -0.5, 1.0, ((0, 16), (1, 32))),
        "slab_ranks": set_ends(jax.random.randint(splits[2], (MT, NT), (5 * R) // 8, R + 1), jax.random.fold_in(splits[2], 1), (5 * R) // 8, R).astype(jnp.int32),
        "panel_left": gaussian(splits[3], (MT, B, R), 1.0, 6.0, ((0, 16), (1, 32))),
        "panel_right": gaussian(splits[4], (MT, B, R), B ** -0.5, 0.125, ((0, 16), (1, 32))),
        "panel_ranks": set_ends(jax.random.randint(splits[5], (MT,), (5 * R) // 8, R + 1), jax.random.fold_in(splits[5], 1), (5 * R) // 8, R).astype(jnp.int32),
        "inverse_factor": draw_inverse_factor(jax.random.fold_in(splits[8], 71), 0),
        "sketch": gaussian(splits[7], (B, R), 1.0, 6.0),
    }


highest = lax.Precision.HIGHEST
shift_rate = 0.01
tiny_shift = 1e-06
factor_scale = 0.5

def product(first_matrix, second_matrix):
    return jnp.matmul(first_matrix, second_matrix, precision=highest)

def flipped(matrix):
    return jnp.swapaxes(matrix, -1, -2)

def apply_tile(outer_left, outer_right, update_left, update_core, update_right, vectors):
    direct = product(outer_left, product(flipped(outer_right), vectors))
    update = product(update_left, product(update_core, product(flipped(update_right), vectors)))
    return direct - update

def orthonormal(vectors):
    gram_matrix = product(flipped(vectors), vectors)
    shift_value = shift_rate * jnp.trace(gram_matrix, axis1=-2, axis2=-1) / gram_matrix.shape[-1] + tiny_shift
    identity = jnp.eye(gram_matrix.shape[-1], dtype=gram_matrix.dtype)
    lower_factor = jnp.linalg.cholesky(gram_matrix + shift_value[..., None, None] * identity)
    solved_rows = lax.linalg.triangular_solve(lower_factor, flipped(vectors), left_side=True, lower=True)
    return flipped(solved_rows)

def recompress(slab_factor, masked_right, row_factor, core_block, column_factor, sketch_float):
    core_flipped = flipped(core_block)

    def forward(vectors):
        return apply_tile(slab_factor, masked_right, row_factor, core_block, column_factor, vectors)

    def backward(vectors):
        return apply_tile(masked_right, slab_factor, column_factor, core_flipped, row_factor, vectors)
    basis_now = orthonormal(forward(sketch_float))
    basis_now = orthonormal(forward(backward(basis_now)))
    projected = backward(basis_now)
    factor_size = factor_scale * math.sqrt(slab_factor.shape[-2])
    return (basis_now * factor_size, projected / factor_size)

def cyclic(total_count, group_count):
    per_group = total_count // group_count
    places = jnp.arange(total_count, dtype=jnp.int32)
    return places % per_group * group_count + places // per_group

def reference(slab_left, slab_right, slab_ranks, panel_left, panel_right, panel_ranks, inverse_factor, sketch):
    row_ids = cyclic(MT, N_ROW)
    col_ids = cyclic(NT, N_COL)
    panel_keep = jnp.arange(R, dtype=jnp.int32)[None, :] < panel_ranks[:, None]
    masked_panel = jnp.where(panel_keep[:, None, :], panel_right, jnp.zeros((), jnp.bfloat16))
    solved = jnp.einsum('ab,pbr->par', inverse_factor.astype(jnp.float32), masked_panel.astype(jnp.float32), precision=highest).astype(jnp.bfloat16)
    where_col = (col_ids % N_ROW * TR + col_ids // N_ROW).astype(jnp.int32)
    column_factor = panel_left[where_col].astype(jnp.float32)
    column_solved = solved[where_col].astype(jnp.float32)
    sketch_float = sketch.astype(jnp.float32)

    def one_row(row_item):
        left_tiles, right_tiles, row_ranks, row_left, row_solved, row_id = row_item
        column_keep = jnp.arange(R, dtype=jnp.int32)[None, :] < row_ranks[:, None]
        masked_right = jnp.where(column_keep[:, None, :], right_tiles.astype(jnp.float32), 0.0)
        core_block = jnp.einsum('br,nbs->nrs', row_solved.astype(jnp.float32), column_solved, precision=highest)
        fresh_left, fresh_right = recompress(left_tiles.astype(jnp.float32), masked_right, row_left.astype(jnp.float32), core_block, column_factor, sketch_float)
        live_tile = (row_id > col_ids)[:, None, None]
        return (jnp.where(live_tile, fresh_left, 0.0).astype(jnp.bfloat16), jnp.where(live_tile, fresh_right, 0.0).astype(jnp.bfloat16))
    new_left, new_right = lax.map(one_row, (slab_left, slab_right, slab_ranks, panel_left, solved, row_ids))
    return (new_left, new_right)
```

```python
import functools
import math

import jax
import jax.numpy as jnp
from jax import lax
from jax.experimental import pallas as pl
from jax.experimental.pallas import tpu as pltpu
from jax.sharding import PartitionSpec as P

MESH = pl.DeviceIdType.MESH
HIGHEST = lax.Precision.HIGHEST
f32 = jnp.float32
bf16 = jnp.bfloat16
shift_rate = 0.01
tiny_shift = 1e-06
factor_scale = 0.5
RANK = 32
TILES = 4
ORDER = (0, 2, 1, 3)


def exchange_kernel(
    rows, cols,
    ranks_ref, left_ref, right_ref, inverse_ref,
    full_left, full_solved, column_left, column_solved,
    half_in, masked, partial, arrived, total, left_block, solved_block, left_column, solved_column,
    half_send, half_recv, part_send, part_recv, left_send, left_recv, solved_send, solved_recv,
    zl_send, zl_recv, zs_send, zs_recv, al_send, al_recv, as_send, as_recv,
):
    row, col = lax.axis_index("row"), lax.axis_index("col")
    chips = cols // 2
    chip, core = col // 2, lax.rem(col, 2)
    partner = col + 1 - 2 * core

    def plane(d):
        return lax.rem(col + d, cols)

    def line(d):
        return lax.rem(row + d, rows)

    def each(lo, hi, body):
        def step(d, carry):
            body(d)
            return carry

        lax.fori_loop(lo, hi, step, 0)

    def copy(src, dst, send, recv, where):
        return pltpu.make_async_remote_copy(
            src_ref=src, dst_ref=dst, send_sem=send, recv_sem=recv,
            device_id=where, device_id_type=MESH,
        )

    barrier = pltpu.get_barrier_semaphore()
    each(1, rows, lambda d: pl.semaphore_signal(
        barrier, inc=1, device_id=(line(d), col), device_id_type=MESH))
    each(1, cols, lambda d: pl.semaphore_signal(
        barrier, inc=1, device_id=(row, plane(d)), device_id_type=MESH))

    index = lax.broadcasted_iota(jnp.int32, (RANK, 1), 0)
    for place, tile in enumerate(ORDER):
        keep = index < ranks_ref[tile]
        masked[place * RANK:(place + 1) * RANK, :] = jnp.where(
            keep, right_ref[tile].astype(f32), 0.0).astype(bf16)
    partial[...] = jnp.dot(masked[...], inverse_ref[...], preferred_element_type=f32)

    pl.semaphore_wait(barrier, rows + cols - 2)

    halves = [
        copy(left_ref.at[1 - core + 2 * k], half_in.at[k], half_send.at[k], half_recv.at[k],
             (row, partner))
        for k in range(2)
    ]
    for h in halves:
        h.start()

    own_rows = pl.ds(pl.multiple_of(core * 64, 64), 64)
    own_lanes = pl.ds(pl.multiple_of(chip * 128, 128), 128)

    def part_copy(d):
        there = plane(d)
        src = partial.at[
            pl.ds(pl.multiple_of(lax.rem(there, 2) * 64, 64), 64),
            pl.ds(pl.multiple_of((there // 2) * 128, 128), 128),
        ]
        return copy(src, arrived.at[d], part_send.at[d], part_recv.at[d], (row, there))

    def sends_part(d, act):
        @pl.when(plane(d) // 2 >= chip)
        def _():
            act(d)

    def takes_part(d, act):
        @pl.when(lax.rem(col + cols - d, cols) // 2 <= chip)
        def _():
            act(d)

    def gather_copy(block, full, send, recv, d):
        return copy(block, full.at[own_rows, own_lanes], send.at[d], recv.at[d], (row, plane(d)))

    def line_copy(block, column, send, recv, d):
        return copy(block.at[0:RANK], column.at[d], send.at[d], recv.at[d], (line(d), col))

    def left_copy(d):
        return gather_copy(left_block, full_left, left_send, left_recv, d)

    def solved_copy(d):
        return gather_copy(solved_block, full_solved, solved_send, solved_recv, d)

    def zl_copy(d):
        return line_copy(left_block, left_column, zl_send, zl_recv, d)

    def zs_copy(d):
        return line_copy(solved_block, solved_column, zs_send, zs_recv, d)

    each(1, cols, lambda d: sends_part(d, lambda d: part_copy(d).start()))

    for h in halves:
        h.wait_recv()
    own = jnp.concatenate([left_ref[core], left_ref[2 + core]], axis=0).astype(f32)
    other = jnp.concatenate([half_in[0], half_in[1]], axis=0).astype(f32)
    block = jnp.where(
        core == 0, jnp.concatenate([own, other], axis=1), jnp.concatenate([other, own], axis=1)
    ).astype(bf16)
    left_block[...] = block
    full_left[own_rows, own_lanes] = block
    left_column[0] = block[0:RANK]
    each(1, rows, lambda d: zl_copy(d).start())
    each(1, cols, lambda d: left_copy(d).start())

    total[...] = partial[own_rows, own_lanes]

    def add_part(d):
        part_copy(d).wait_recv()
        total[...] += arrived[d]

    each(1, cols, lambda d: takes_part(d, add_part))
    block = total[...].astype(bf16)
    solved_block[...] = block
    full_solved[own_rows, own_lanes] = block
    solved_column[0] = block[0:RANK]
    each(1, rows, lambda d: zs_copy(d).start())
    each(1, cols, lambda d: solved_copy(d).start())

    def column_copy(column, out, send, recv, d):
        there = lax.rem(row + rows - d, rows) + rows * core
        return there, copy(
            column.at[d], out.at[:, own_lanes], send.at[d], recv.at[chip], (row, there))

    def send_columns(column, out, send, recv):
        def one(d):
            there, c = column_copy(column, out, send, recv, d)

            @pl.when(there != col)
            def _():
                c.start()

            @pl.when(there == col)
            def _():
                out[:, own_lanes] = column[d]

        each(0, rows, one)

    def sent_columns(column, out, send, recv):
        def one(d):
            there, c = column_copy(column, out, send, recv, d)

            @pl.when(there != col)
            def _():
                c.wait_send()

        each(0, rows, one)

    def take_columns(column, out, send, recv):
        def one(x):
            lanes = pl.ds(pl.multiple_of(x * 128, 128), 128)

            @pl.when(2 * x + col // rows != col)
            def _():
                copy(column.at[0], out.at[:, lanes], send.at[0], recv.at[x],
                     (row, partner)).wait_recv()

        each(0, chips, one)

    each(1, rows, lambda d: zl_copy(d).wait_recv())
    send_columns(left_column, column_left, al_send, al_recv)
    each(1, rows, lambda d: zs_copy(d).wait_recv())
    send_columns(solved_column, column_solved, as_send, as_recv)

    each(1, cols, lambda d: left_copy(d).wait_recv())
    each(1, cols, lambda d: solved_copy(d).wait_recv())
    take_columns(left_column, column_left, al_send, al_recv)
    take_columns(solved_column, column_solved, as_send, as_recv)

    for h in halves:
        h.wait_send()
    each(1, cols, lambda d: sends_part(d, lambda d: part_copy(d).wait_send()))
    each(1, cols, lambda d: left_copy(d).wait_send())
    each(1, cols, lambda d: solved_copy(d).wait_send())
    each(1, rows, lambda d: zl_copy(d).wait_send())
    each(1, rows, lambda d: zs_copy(d).wait_send())
    sent_columns(left_column, column_left, al_send, al_recv)
    sent_columns(solved_column, column_solved, as_send, as_recv)


def exchange(rows, cols, ranks, left, right, inverse):
    size = inverse.shape[1]
    vmem = pl.BlockSpec(memory_space=pltpu.VMEM)
    dma = pltpu.SemaphoreType.DMA
    wide = TILES * RANK
    sems = [2, 2] + [cols] * 6 + [rows] * 8
    return pl.pallas_call(
        functools.partial(exchange_kernel, rows, cols),
        out_shape=(
            jax.ShapeDtypeStruct((wide, size), bf16),
            jax.ShapeDtypeStruct((wide, size), bf16),
            jax.ShapeDtypeStruct((RANK, size), bf16),
            jax.ShapeDtypeStruct((RANK, size), bf16),
        ),
        in_specs=[pl.BlockSpec(memory_space=pltpu.SMEM), vmem, vmem, vmem],
        out_specs=(vmem, vmem, vmem, vmem),
        scratch_shapes=[
            pltpu.VMEM((2, RANK, 64), bf16),
            pltpu.VMEM((wide, 64), bf16),
            pltpu.VMEM((wide, size), f32),
            pltpu.VMEM((cols, 64, 128), f32),
            pltpu.VMEM((64, 128), f32),
            pltpu.VMEM((64, 128), bf16),
            pltpu.VMEM((64, 128), bf16),
            pltpu.VMEM((rows, RANK, 128), bf16),
            pltpu.VMEM((rows, RANK, 128), bf16),
        ] + [dma((n,)) for n in sems],
        compiler_params=pltpu.CompilerParams(collective_id=0, has_side_effects=True),
        name="exchange",
    )(ranks, left, right, inverse)


def product(a, b, contract=((1,), (0,))):
    return lax.dot_general(a, b, (contract, ((), ())), precision=HIGHEST,
                           preferred_element_type=f32)


def gram(a, b):
    return lax.dot_general(a, b, (((1,), (1,)), ((), ())), preferred_element_type=f32)


NT = ((1,), (1,))
TN = ((0,), (0,))


def inverse_root(matrix):
    wide = TILES * RANK
    lane = lax.broadcasted_iota(jnp.int32, (RANK, wide), 1)
    sub = lax.broadcasted_iota(jnp.int32, (RANK, wide), 0)
    group = (lane // RANK) * RANK
    eye = jnp.where(lane - group == sub, 1.0, 0.0).astype(f32)
    g = matrix[0:RANK]
    for t in range(1, TILES):
        g = g + matrix[t * RANK:(t + 1) * RANK]
    diagonal = jnp.sum(g * eye, axis=0, keepdims=True)
    same = jnp.where(
        lax.broadcasted_iota(jnp.int32, (wide, wide), 0) // RANK
        == lax.broadcasted_iota(jnp.int32, (wide, wide), 1) // RANK, 1.0, 0.0).astype(f32)
    trace = product(diagonal, same)
    g = g + (shift_rate * trace / RANK + tiny_shift) * eye
    e = eye
    pivots = jnp.zeros((RANK, wide), f32)
    for k in range(RANK):
        column = jnp.take_along_axis(g, group + k, axis=1, mode="promise_in_bounds")
        pivot = column[k:k + 1]
        pivots = jnp.where(sub == k, pivot, pivots)
        if k < RANK - 1:
            m = jnp.where(sub > k, column / pivot, 0.0)
            g = g - m * g[k:k + 1]
            e = e - m * e[k:k + 1]
    compact = e * lax.rsqrt(pivots)
    return jnp.concatenate([compact] * TILES, axis=0) * same


def split(x):
    high = x.astype(bf16)
    return high, (x - high.astype(f32)).astype(bf16)


def recompress_kernel(
    ranks_ref, live_ref, slab_left, slab_right, left_ref, solved_ref, column_left, column_solved,
    sketch_ref, new_left, new_right, left_in, right_in,
):
    wide = TILES * RANK
    size = sketch_ref.shape[1]
    index = lax.broadcasted_iota(jnp.int32, (RANK, 1), 0)
    for place, tile in enumerate(ORDER):
        keep = index < ranks_ref[tile, 0]
        at = slice(place * RANK, (place + 1) * RANK)
        left_in[at, :] = slab_left[tile, 0]
        right_in[at, :] = jnp.where(keep, slab_right[tile, 0].astype(f32), 0.0).astype(bf16)

    def square(n):
        a = lax.broadcasted_iota(jnp.int32, (n, n), 0)
        b = lax.broadcasted_iota(jnp.int32, (n, n), 1)
        return jnp.where((a % wide) // RANK == (b % wide) // RANK, 1.0, 0.0).astype(f32)

    same = square(wide)

    u, v, p = left_in[...], right_in[...], left_ref[...]
    pc, sk = column_left[...], sketch_ref[...]
    core = gram(solved_ref[...], column_solved[...])
    up = gram(u, p) * same
    left_gram = jnp.concatenate([
        jnp.concatenate([gram(u, u) * same, up], axis=1),
        jnp.concatenate([up.T, gram(p, p) * same], axis=1),
    ], axis=0)
    v_v, v_pc, pc_pc = gram(v, v), gram(v, pc), gram(pc, pc)
    v_s, pc_s = gram(v, sk), gram(pc, sk)

    def blocks(x):
        return jnp.concatenate([x] * TILES, axis=1) * same

    cross = product(v_pc, core, NT) * -same
    right_gram = jnp.concatenate([
        jnp.concatenate([v_v * same, cross], axis=1),
        jnp.concatenate([cross.T, product(product(core, pc_pc), core, NT) * same], axis=1),
    ], axis=0)
    x0 = jnp.concatenate([blocks(v_s), blocks(-product(core, pc_s))], axis=0)
    y0 = product(left_gram, x0)
    root0 = inverse_root(product(x0, y0, TN))
    x1 = product(right_gram, product(y0, root0, NT))
    y1 = product(left_gram, x1)
    root1 = inverse_root(product(x1, y1, TN))
    z1 = product(x1, root1, NT)
    w1 = product(y1, root1, NT)
    scale = factor_scale * math.sqrt(size)
    w_low = -product(core, w1[wide:], TN)
    zl = z1 * scale
    w_top = w1[:wide] * (1.0 / scale)
    w_low = w_low * (1.0 / scale)
    zu = jnp.concatenate(split(zl[:wide]), axis=1)
    zp = jnp.concatenate(split(zl[wide:]), axis=1)
    wv = jnp.concatenate(split(w_top), axis=1)
    wc = jnp.concatenate(split(w_low), axis=1)

    def tn(a, b):
        return lax.dot_general(a, b, (TN, ((), ())), preferred_element_type=f32)

    chunk = min(512, size)
    for at in range(0, size, chunk):
        lanes = slice(at, at + chunk)
        q = tn(zu, left_in[:, lanes]) + tn(zp, left_ref[:, lanes])
        r = tn(wv, right_in[:, lanes]) + tn(wc, column_left[:, lanes])
        q = (q[:wide] + q[wide:]).astype(bf16)
        r = (r[:wide] + r[wide:]).astype(bf16)
        for place, tile in enumerate(ORDER):
            rows = slice(place * RANK, (place + 1) * RANK)
            live = live_ref[tile] > 0
            zero = jnp.zeros((RANK, chunk), f32)
            new_left[tile, 0, :, lanes] = jnp.where(live, q[rows].astype(f32), zero).astype(bf16)
            new_right[tile, 0, :, lanes] = jnp.where(live, r[rows].astype(f32), zero).astype(bf16)


def recompress(ranks, live, slab_left, slab_right, left, solved, column_left, column_solved, sketch):
    vmem = pl.BlockSpec(memory_space=pltpu.VMEM)
    smem = pl.BlockSpec(memory_space=pltpu.SMEM)
    wide, size = left.shape
    out = jax.ShapeDtypeStruct(slab_left.shape, bf16)
    return pl.pallas_call(
        recompress_kernel,
        out_shape=(out, out),
        in_specs=[smem, smem] + [vmem] * 7,
        out_specs=(vmem, vmem),
        scratch_shapes=[pltpu.VMEM((wide, size), bf16), pltpu.VMEM((wide, size), bf16)],
        name="recompress",
    )(ranks, live, slab_left, slab_right, left, solved, column_left, column_solved, sketch)


def shards(
    slab_left, slab_right, slab_ranks, panel_left, panel_right, panel_ranks, inverse_factor, sketch
):
    rows, cols = lax.axis_size("row"), lax.axis_size("col")

    def flip(x):
        return jnp.swapaxes(x, -1, -2)

    left, solved, column_left, column_solved = exchange(
        rows, cols, panel_ranks, flip(panel_left), flip(panel_right), flip(inverse_factor))
    ids = jnp.arange(TILES, dtype=jnp.int32) * rows + lax.axis_index("row")
    live = (ids > lax.axis_index("col")).astype(jnp.int32)
    new_left, new_right = recompress(
        slab_ranks, live, flip(slab_left), flip(slab_right), left, solved, column_left,
        column_solved, flip(sketch))
    return flip(new_left), flip(new_right)


def solution(mesh):
    placed = (
        P("row", "col", None, None),
        P("row", "col", None, None),
        P("row", "col"),
        P("row", "col", None),
        P("row", "col", None),
        P("row"),
        P(None, "col"),
        P(),
    )
    return jax.shard_map(
        shards,
        mesh=mesh,
        in_specs=placed,
        out_specs=(P("row", "col", None, None), P("row", "col", None, None)),
        check_vma=False,
    )
```

```python
import functools
import math

import jax
import jax.numpy as jnp
from jax import lax
from jax.experimental import pallas as pl
from jax.experimental.pallas import tpu as pltpu
from jax.sharding import PartitionSpec as P

MESH = pl.DeviceIdType.MESH
HIGHEST = lax.Precision.HIGHEST
f32 = jnp.float32
bf16 = jnp.bfloat16
shift_rate = 0.01
tiny_shift = 1e-06
factor_scale = 0.5
RANK = 32
TILES = 4
ORDER = (0, 2, 1, 3)


def exchange_kernel(
    rows, cols,
    ranks_hbm, left_hbm, right_hbm, inverse_hbm, tile_ranks_hbm, slab_left, slab_right, sketch_hbm,
    full_left, column_left, rows_left, rows_right, left_gram, right_gram, mixed_gram, core_block,
    ranks_ref, tile_ranks, left_ref, right_ref, inverse_ref, sketch_ref, slab_v, load_sem,
    full_solved, column_solved,
    left_in, right_in, inverse_in, partial, arrived, total,
    left_block, solved_block,
    pair_send, pair_recv, part_send, part_recv, left_send, left_recv, solved_send, solved_recv,
    pass_send, pass_recv,
    cl_send, cl_recv, cs_send, cs_recv,
):
    row, col = lax.axis_index("row"), lax.axis_index("col")
    chips = cols // 2
    chip, core = col // 2, lax.rem(col, 2)
    partner = col + 1 - 2 * core

    def line(d):
        return lax.rem(row + d, rows)

    def each(lo, hi, body):
        def step(d, carry):
            body(d)
            return carry

        lax.fori_loop(lo, hi, step, 0)

    def copy(src, dst, send, recv, where):
        return pltpu.make_async_remote_copy(
            src_ref=src, dst_ref=dst, send_sem=send, recv_sem=recv,
            device_id=where, device_id_type=MESH,
        )

    barrier = pltpu.get_barrier_semaphore()
    root, root_core = lax.rem(col, rows), col // rows
    keeps = jnp.logical_and(row == root, core == root_core)

    def hello(to_row, to_col):
        pl.semaphore_signal(barrier, inc=1, device_id=(to_row, to_col), device_id_type=MESH)

    def greet_source(x):
        @pl.when(jnp.logical_not(jnp.logical_and(keeps, x == chip)))
        def _():
            hello(root, 2 * x + root_core)

    each(0, chips, greet_source)
    each(1, chips, lambda d: hello(row, 2 * lax.rem(chip + d, chips) + core))
    hello(row, partner)

    loads = [
        pltpu.make_async_copy(src, dst, load_sem.at[n])
        for n, (src, dst) in enumerate((
            (ranks_hbm, ranks_ref), (right_hbm, right_ref), (inverse_hbm, inverse_ref),
            (left_hbm, left_ref), (tile_ranks_hbm, tile_ranks), (sketch_hbm, sketch_ref),
            (slab_right, slab_v),
        ))
    ] + [
        pltpu.make_async_copy(
            slab_left.at[tile, 0], rows_left.at[place * RANK:(place + 1) * RANK],
            load_sem.at[7 + place])
        for place, tile in enumerate(ORDER)
    ]
    for c in loads:
        c.start()
    for c in loads[:4]:
        c.wait()

    index = lax.broadcasted_iota(jnp.int32, (RANK, 1), 0)

    def masked(first, second):
        return jnp.concatenate([
            jnp.where(index < ranks_ref[core + 2 * k], x.astype(f32), 0.0)
            for k, x in enumerate((first, second))
        ], axis=0).astype(bf16)

    partial[...] = jnp.dot(
        masked(right_ref[core], right_ref[2 + core]), inverse_ref[...],
        preferred_element_type=f32)

    pl.semaphore_wait(barrier, rows + chips - jnp.where(keeps, 1, 0))

    ends = (row, partner)
    pairs = [copy(inverse_ref, inverse_in, pair_send.at[0], pair_recv.at[0], ends)]
    for k in range(2):
        pairs.append(copy(
            right_ref.at[1 - core + 2 * k], right_in.at[k],
            pair_send.at[1 + k], pair_recv.at[1 + k], ends))
    for k in range(2):
        pairs.append(copy(
            left_ref.at[1 - core + 2 * k], left_in.at[k],
            pair_send.at[3 + k], pair_recv.at[3 + k], ends))
    for c in pairs[1:] + pairs[:1]:
        c.start()

    own_rows = pl.ds(pl.multiple_of(core * 64, 64), 64)

    def lanes_of(x):
        return pl.ds(pl.multiple_of(x * 128, 128), 128)

    own_lanes = lanes_of(chip)

    def there(d):
        return lax.rem(chip + d, chips)

    def part_copy(d):
        return copy(partial.at[:, lanes_of(there(d))], arrived.at[d], part_send.at[d],
                    part_recv.at[d], (row, 2 * there(d) + core))

    def sends_part(d, act):
        @pl.when(there(d) > chip)
        def _():
            act(d)

    def takes_part(d, act):
        @pl.when(lax.rem(chip + chips - d, chips) < chip)
        def _():
            act(d)

    def gather_copy(block, full, send, recv, d):
        return copy(block, full.at[own_rows, own_lanes], send.at[d], recv.at[d],
                    (row, 2 * there(d) + core))

    target = row + rows * core

    def column_copy(block, out, send, recv, d):
        return copy(block.at[0:RANK], out.at[:, own_lanes], send.at[d], recv.at[chip],
                    (line(d), target))

    def sends_column(d, act):
        @pl.when(jnp.logical_not(jnp.logical_and(keeps, d == 0)))
        def _():
            act(d)

    def send_columns(block, out, send, recv):
        each(0, rows, lambda d: sends_column(
            d, lambda d: column_copy(block, out, send, recv, d).start()))

        @pl.when(keeps)
        def _():
            out[:, own_lanes] = block[0:RANK]

    def sent_columns(block, out, send, recv):
        each(0, rows, lambda d: sends_column(
            d, lambda d: column_copy(block, out, send, recv, d).wait_send()))

    def take_columns(block, out, send, recv):
        def one(x):
            @pl.when(jnp.logical_not(jnp.logical_and(keeps, x == chip)))
            def _():
                copy(block.at[0:RANK], out.at[:, lanes_of(x)], send.at[0], recv.at[x],
                     ends).wait_recv()

        each(0, chips, one)

    def left_copy(d):
        return gather_copy(left_block, full_left, left_send, left_recv, d)

    def solved_copy(d):
        return gather_copy(solved_block, full_solved, solved_send, solved_recv, d)

    for c in pairs[1:]:
        c.wait_recv()
    own = jnp.concatenate([left_ref[core], left_ref[2 + core]], axis=0).astype(f32)
    other = jnp.concatenate([left_in[0], left_in[1]], axis=0).astype(f32)
    block = jnp.where(
        core == 0, jnp.concatenate([own, other], axis=1), jnp.concatenate([other, own], axis=1)
    ).astype(bf16)
    left_block[...] = block
    full_left[own_rows, own_lanes] = block
    send_columns(left_block, column_left, cl_send, cl_recv)
    pairs[0].wait_recv()
    partial[...] += jnp.dot(
        masked(right_in[0], right_in[1]), inverse_in[...], preferred_element_type=f32)
    each(1, chips, lambda d: sends_part(d, lambda d: part_copy(d).start()))

    for c in loads[4:]:
        c.wait()
    for place, tile in enumerate(ORDER):
        keep = index < tile_ranks[tile]
        rows_right[place * RANK:(place + 1) * RANK, :] = jnp.where(
            keep, slab_v[tile, 0].astype(f32), 0.0).astype(bf16)
    wide = TILES * RANK
    same = same_tile()
    left_gram[0:wide, 0:wide] = gram(rows_left[...], rows_left[...]) * same
    right_gram[...] = gram(rows_right[...], rows_right[...]) * same
    mixed_gram[0:wide, 0:RANK] = gram(rows_right[...], sketch_ref[...])

    total[...] = partial[:, own_lanes]

    def add_part(d):
        part_copy(d).wait_recv()
        total[...] += arrived[d]

    each(1, chips, lambda d: takes_part(d, add_part))
    block = total[...].astype(bf16)
    solved_block[...] = block
    full_solved[own_rows, own_lanes] = block
    send_columns(solved_block, column_solved, cs_send, cs_recv)
    each(1, chips, lambda d: solved_copy(d).start())
    each(1, chips, lambda d: left_copy(d).start())

    def pass_on(full, k):
        part = full.at[own_rows, :]
        return copy(part, part, pass_send.at[k], pass_recv.at[k], ends)

    each(1, chips, lambda d: solved_copy(d).wait_recv())
    pass_on(full_solved, 0).start()
    each(1, chips, lambda d: left_copy(d).wait_recv())
    pass_on(full_left, 1).start()

    take_columns(left_block, column_left, cl_send, cl_recv)
    low = slice(wide, wide + RANK)
    mixed_gram[low, 0:RANK] = gram(column_left[...], sketch_ref[...])
    mixed_gram[0:wide, RANK:2 * RANK] = gram(rows_right[...], column_left[...])
    mixed_gram[low, RANK:2 * RANK] = gram(column_left[...], column_left[...])
    pass_on(full_left, 1).wait_recv()
    left_gram[0:wide, wide:2 * wide] = gram(rows_left[...], full_left[...]) * same
    left_gram[wide:2 * wide, 0:wide] = gram(full_left[...], rows_left[...]) * same
    left_gram[wide:2 * wide, wide:2 * wide] = gram(full_left[...], full_left[...]) * same
    pass_on(full_solved, 0).wait_recv()
    take_columns(solved_block, column_solved, cs_send, cs_recv)
    core_block[...] = gram(full_solved[...], column_solved[...])

    for c in pairs:
        c.wait_send()
    each(1, chips, lambda d: sends_part(d, lambda d: part_copy(d).wait_send()))
    each(1, chips, lambda d: left_copy(d).wait_send())
    each(1, chips, lambda d: solved_copy(d).wait_send())
    sent_columns(left_block, column_left, cl_send, cl_recv)
    sent_columns(solved_block, column_solved, cs_send, cs_recv)
    pass_on(full_solved, 0).wait_send()
    pass_on(full_left, 1).wait_send()


def exchange(rows, cols, ranks, left, right, inverse, tile_ranks, slab_left, slab_right, sketch):
    size = inverse.shape[1]
    vmem = pl.BlockSpec(memory_space=pltpu.VMEM)
    hbm = pl.BlockSpec(memory_space=pltpu.HBM)
    dma = pltpu.SemaphoreType.DMA
    wide = TILES * RANK
    sems = [5, 5] + [cols // 2] * 6 + [2, 2] + [rows, cols // 2] * 2
    shape = jax.ShapeDtypeStruct
    return pl.pallas_call(
        functools.partial(exchange_kernel, rows, cols),
        out_shape=(
            shape((wide, size), bf16),
            shape((RANK, size), bf16),
            shape((wide, size), bf16),
            shape((wide, size), bf16),
            shape((2 * wide, 2 * wide), f32),
            shape((wide, wide), f32),
            shape((wide + RANK, 2 * RANK), f32),
            shape((wide, RANK), f32),
        ),
        in_specs=[hbm] * 8,
        out_specs=(vmem,) * 8,
        scratch_shapes=[
            pltpu.SMEM(ranks.shape, jnp.int32),
            pltpu.SMEM(tile_ranks.shape, jnp.int32),
            pltpu.VMEM(left.shape, bf16),
            pltpu.VMEM(right.shape, bf16),
            pltpu.VMEM(inverse.shape, bf16),
            pltpu.VMEM(sketch.shape, bf16),
            pltpu.VMEM(slab_right.shape, bf16),
            dma((11,)),
            pltpu.VMEM((wide, size), bf16),
            pltpu.VMEM((RANK, size), bf16),
            pltpu.VMEM((2, RANK, 64), bf16),
            pltpu.VMEM((2, RANK, 64), bf16),
            pltpu.VMEM((64, size), bf16),
            pltpu.VMEM((64, size), f32),
            pltpu.VMEM((cols // 2, 64, 128), f32),
            pltpu.VMEM((64, 128), f32),
            pltpu.VMEM((64, 128), bf16),
            pltpu.VMEM((64, 128), bf16),
        ] + [dma((n,)) for n in sems],
        compiler_params=pltpu.CompilerParams(
            collective_id=0, has_side_effects=True),
        name="exchange",
    )(ranks, left, right, inverse, tile_ranks, slab_left, slab_right, sketch)


def same_tile():
    wide = TILES * RANK
    a = lax.broadcasted_iota(jnp.int32, (wide, wide), 0)
    b = lax.broadcasted_iota(jnp.int32, (wide, wide), 1)
    return jnp.where(a // RANK == b // RANK, 1.0, 0.0).astype(f32)


def product(a, b, contract=((1,), (0,))):
    return lax.dot_general(a, b, (contract, ((), ())), precision=HIGHEST,
                           preferred_element_type=f32)


def gram(a, b):
    return lax.dot_general(a, b, (((1,), (1,)), ((), ())), preferred_element_type=f32)


NT = ((1,), (1,))
TN = ((0,), (0,))


def inverse_root(matrix):
    wide = TILES * RANK
    lane = lax.broadcasted_iota(jnp.int32, (RANK, wide), 1)
    sub = lax.broadcasted_iota(jnp.int32, (RANK, wide), 0)
    group = (lane // RANK) * RANK
    eye = jnp.where(lane - group == sub, 1.0, 0.0).astype(f32)
    g = matrix[0:RANK]
    for t in range(1, TILES):
        g = g + matrix[t * RANK:(t + 1) * RANK]
    diagonal = jnp.sum(g * eye, axis=0, keepdims=True)
    same = same_tile()
    trace = product(diagonal, same)
    g = g + (shift_rate * trace / RANK + tiny_shift) * eye
    e = eye
    pivots = jnp.zeros((RANK, wide), f32)

    def spread(k):
        return jnp.take_along_axis(g, group + k, axis=1, mode="promise_in_bounds")

    column = spread(0)
    for k in range(RANK):
        pivot = column[k:k + 1]
        pivots = jnp.where(sub == k, pivot, pivots)
        if k < RANK - 1:
            m = jnp.where(sub > k, column * (1.0 / pivot), 0.0)
            column = spread(k + 1) - m * column[k + 1:k + 2]
            g = g - m * g[k:k + 1]
            e = e - m * e[k:k + 1]
    compact = e * lax.rsqrt(pivots)
    return jnp.concatenate([compact] * TILES, axis=0) * same


def split(x):
    high = x.astype(bf16)
    return high, (x - high.astype(f32)).astype(bf16)


def recompress_kernel(
    left_ref, column_left, left_in, right_in, left_gram_ref, right_ref, mixed, core_ref,
    new_left, new_right,
):
    wide = TILES * RANK
    size = left_ref.shape[1]
    same = same_tile()
    core, left_gram = core_ref[...], left_gram_ref[...]
    v_s, v_pc = mixed[0:wide, 0:RANK], mixed[0:wide, RANK:2 * RANK]
    pc_s, pc_pc = mixed[wide:wide + RANK, 0:RANK], mixed[wide:wide + RANK, RANK:2 * RANK]

    def blocks(x):
        return jnp.concatenate([x] * TILES, axis=1) * same

    cross = product(v_pc, core, NT) * -same
    right_gram = jnp.concatenate([
        jnp.concatenate([right_ref[...], cross], axis=1),
        jnp.concatenate([cross.T, product(product(core, pc_pc), core, NT) * same], axis=1),
    ], axis=0)
    x0 = jnp.concatenate([blocks(v_s), blocks(-product(core, pc_s))], axis=0)
    y0 = product(left_gram, x0)
    root0 = inverse_root(product(x0, y0, TN))
    x1 = product(right_gram, product(y0, root0, NT))
    y1 = product(left_gram, x1)
    root1 = inverse_root(product(x1, y1, TN))
    z1 = product(x1, root1, NT)
    w1 = product(y1, root1, NT)
    scale = factor_scale * math.sqrt(size)
    w_low = -product(core, w1[wide:], TN)
    zl = z1 * scale
    w_top = w1[:wide] * (1.0 / scale)
    w_low = w_low * (1.0 / scale)
    zu = jnp.concatenate(split(zl[:wide]), axis=1)
    zp = jnp.concatenate(split(zl[wide:]), axis=1)
    wv = jnp.concatenate(split(w_top), axis=1)
    wc = jnp.concatenate(split(w_low), axis=1)

    def tn(a, b):
        return lax.dot_general(a, b, (TN, ((), ())), preferred_element_type=f32)

    chunk = min(512, size)
    for at in range(0, size, chunk):
        lanes = slice(at, at + chunk)
        q = tn(zu, left_in[:, lanes]) + tn(zp, left_ref[:, lanes])
        r = tn(wv, right_in[:, lanes]) + tn(wc, column_left[:, lanes])
        q = (q[:wide] + q[wide:]).astype(bf16)
        r = (r[:wide] + r[wide:]).astype(bf16)
        for place, tile in enumerate(ORDER):
            rows = slice(place * RANK, (place + 1) * RANK)
            live = tile * lax.axis_size("row") + lax.axis_index("row") > lax.axis_index("col")
            zero = jnp.zeros((RANK, chunk), f32)
            new_left[tile, 0, :, lanes] = jnp.where(live, q[rows].astype(f32), zero).astype(bf16)
            new_right[tile, 0, :, lanes] = jnp.where(live, r[rows].astype(f32), zero).astype(bf16)


def recompress(shape, *parts):
    vmem = pl.BlockSpec(memory_space=pltpu.VMEM)
    out = jax.ShapeDtypeStruct(shape, bf16)
    return pl.pallas_call(
        recompress_kernel,
        out_shape=(out, out),
        in_specs=[vmem] * len(parts),
        out_specs=(vmem, vmem),
        name="recompress",
    )(*parts)


def shards(
    slab_left, slab_right, slab_ranks, panel_left, panel_right, panel_ranks, inverse_factor, sketch
):
    rows, cols = lax.axis_size("row"), lax.axis_size("col")

    def flip(x):
        return jnp.swapaxes(x, -1, -2)

    slab_left, slab_right = flip(slab_left), flip(slab_right)
    parts = exchange(
        rows, cols, panel_ranks, flip(panel_left), flip(panel_right), flip(inverse_factor),
        slab_ranks.reshape(TILES), slab_left, slab_right, flip(sketch))
    new_left, new_right = recompress(slab_left.shape, *parts)
    return flip(new_left), flip(new_right)


def solution(mesh):
    placed = (
        P("row", "col", None, None),
        P("row", "col", None, None),
        P("row", "col"),
        P("row", "col", None),
        P("row", "col", None),
        P("row"),
        P(None, "col"),
        P(),
    )
    return jax.shard_map(
        shards,
        mesh=mesh,
        in_specs=placed,
        out_specs=(P("row", "col", None, None), P("row", "col", None, None)),
        check_vma=False,
    )
```
